32 devices in a mesh: gx: 4 (over x, core), gy: 4 (over z), gz: 2 (over y).
Axes of the slice: x: 2, y: 2, z: 4, core: 2. Of those that a mesh axis runs over, the one named last changes fastest.
Arguments:
- outcomes: bfloat16 [24576, 2048], P(('gx', 'gy', 'gz')), may hold values from -6 to 6
- sketch: bfloat16 [24576, 128], P(('gx', 'gy', 'gz')), may hold values from -6 to 6
Outputs:
- left_basis: float32 [24576, 128], P(('gx', 'gy', 'gz'))
- factor: float32 [128, 128], replicated
The draws below stay inside these ranges and needn't reach their ends.
All inputs are finite; a program needn't handle non-finite values.
Results may differ from the reference program's by a relative error of at most 0.005.
Values may be sent and summed in bfloat16 or wider, within the bound.
A program may use at most 64 MiB of HBM per device.

```python
import math
import jax
import jax.numpy as jnp
from jax import lax

DAYS = 2048
RANK = 128
POWER = 2
UNITS = 24576


def block_scale(own_key, extent, pieces, smallest, high):
    def one(axis_at, blocks):
        heights = jax.random.uniform(jax.random.fold_in(jax.random.fold_in(own_key, 6), axis_at), (blocks,), jnp.float32, smallest / len(pieces), high / len(pieces))
        return jnp.repeat(jnp.exp(heights), extent[axis_at] // blocks).reshape((-1,) + (1,) * (len(extent) - axis_at - 1))

    level = one(*pieces[0])
    for cut in pieces[1:]:
        level = level * one(*cut)
    return level


def centred(own_key, dims, spread, reach, split=(), dtype=jnp.bfloat16):
    gain = block_scale(own_key, dims, split, -0.22, 0.18) if split else 1.0
    drawn = jax.random.normal(own_key, dims, jnp.float32) * spread * gain
    return jnp.minimum(jnp.maximum(drawn, -reach), reach).astype(dtype)


def setup_inputs(seed: int = 0) -> dict:
    splits = jax.random.split(jax.random.key(seed), 3)
    return {
        "outcomes": centred(splits[0], (UNITS, DAYS), 1.0, 6.0, ((0, 32),)),
        "sketch": centred(splits[1], (UNITS, RANK), 1.0, 6.0, ((0, 32),)),
    }


def reference(outcomes, sketch):
    current = sketch
    left_basis = None
    factor = None
    for power_step in range(POWER):
        summed = lax.dot_general(outcomes.astype(jnp.float32), current.astype(jnp.float32), (((0,), (0,)), ((), ())), preferred_element_type=jnp.float32)
        day_weights = (summed / math.sqrt(UNITS)).astype(jnp.bfloat16)
        projected = jnp.dot(outcomes.astype(jnp.float32), day_weights.astype(jnp.float32), preferred_element_type=jnp.float32) / math.sqrt(DAYS)
        gram = jnp.dot(projected.T, projected, precision=lax.Precision.HIGHEST) / UNITS
        lower_tri = jnp.linalg.cholesky(gram)
        left_basis = lax.linalg.triangular_solve(lower_tri, projected, left_side=False, lower=True, transpose_a=True)
        factor = lower_tri.T
        current = left_basis.astype(jnp.bfloat16)
    return (left_basis, factor)
```

```python
import functools
import math

import jax
import jax.numpy as jnp
from jax import lax
from jax.experimental import pallas as pl
from jax.experimental.pallas import tpu as pltpu
from jax.sharding import PartitionSpec as P

POWER = 2
AXES = ("gx", "gy", "gz")
MESH = pl.DeviceIdType.MESH
HIGHEST = lax.Precision.HIGHEST
PANEL = 8


def plan(sizes, days):
    size_x, size_y, size_z = sizes
    plane = (size_x // 2) * size_z
    line = size_y
    half = days // 2
    block = half // plane
    scatter = block % (16 * line) == 0
    piece = block // line if scatter else block
    return plane, line, half, block, scatter, piece


def step_kernel(
    sizes, units, o_ref, c_ref, p_ref, g_ref,
    ct, s_send, s_recv, s_mine, x_recv, z_sum, z_recv, w,
    g_loc, g_recv, g_half, gx_recv, g_plane, gz_recv, g_full,
    c_ss, c_rs, x_ss, x_rs, z_ss, z_rs, az_ss, az_rs, ax_ss, ax_rs, ac_ss, ac_rs,
    gc_ss, gc_rs, gx_ss, gx_rs, gz_ss, gz_rs, gf_ss, gf_rs,
):
    days = o_ref.shape[1]
    rows = o_ref.shape[0]
    rank = c_ref.shape[1]
    plane, line, half, block, scatter, piece = plan(sizes, days)
    size_z = sizes[2]
    ix, iy, iz = (lax.axis_index(a) for a in AXES)
    core = lax.rem(ix, 2)
    q = lax.div(ix, 2) * size_z + iz
    z = iy

    def device(c_at, q_at, z_at):
        return (lax.div(q_at, size_z) * 2 + c_at, z_at, lax.rem(q_at, size_z))

    other = 1 - core
    pair_dev = device(other, q, z)

    def q_to(k):
        return lax.rem(q + k, plane)

    def q_from(k):
        return lax.rem(q + plane - k, plane)

    def z_to(k):
        return lax.rem(z + k, line)

    def z_from(k):
        return lax.rem(z + line - k, line)

    def remote(src, dst, ss, rs, dev):
        return pltpu.make_async_remote_copy(
            src_ref=src, dst_ref=dst, send_sem=ss, recv_sem=rs, device_id=dev, device_id_type=MESH
        )

    partners = [pair_dev]
    partners += [device(core, q_to(k), z) for k in range(1, plane)]
    partners += [device(core, q, z_to(k)) for k in range(1, line)]
    barrier = pltpu.get_barrier_semaphore()
    for dev in partners:
        pl.semaphore_signal(barrier, inc=1, device_id=dev, device_id_type=MESH)

    ct[...] = c_ref[...].astype(jnp.float32).T.astype(jnp.bfloat16)

    def product(dst, side, first, width):
        at = pl.multiple_of(side * half + first, 128)
        part = jnp.dot(ct[...], o_ref[:, pl.ds(at, width)], preferred_element_type=jnp.float32)
        dst[pl.ds(pl.multiple_of(first, 128), width), :] = part.T

    by_block = block % 128 == 0
    sends = []
    order = list(range(1, plane)) + [0]
    if not by_block:
        for first in range(0, half, 256):
            product(s_send, other, first, min(256, half))

    def q_rows(k):
        return pl.multiple_of(q_to(k) * block, block)

    for n, k in enumerate(order):
        at = q_rows(k)
        if by_block:
            product(s_send, other, at, block)
        if n == 0:
            pl.semaphore_wait(barrier, len(partners))
        copy = remote(
            s_send.at[pl.ds(at, block)], s_recv.at[pl.ds(at, block)], c_ss.at[k], c_rs.at[k], pair_dev
        )
        copy.start()
        sends.append(copy)
    if not by_block:
        for first in range(0, half, 256):
            product(s_mine, core, first, min(256, half))
    for k in order:
        at = q_rows(k)
        if by_block:
            product(s_mine, core, at, block)
        mine = s_recv.at[pl.ds(at, block)]
        remote(mine, mine, c_ss.at[k], c_rs.at[k], pair_dev).wait_recv()
        if k:
            s_mine[pl.ds(at, block), :] += s_recv[pl.ds(at, block), :]
            copy = remote(
                s_mine.at[pl.ds(at, block)], x_recv.at[k - 1], x_ss.at[k - 1], x_rs.at[k - 1],
                device(core, q_to(k), z),
            )
            copy.start()
            sends.append(copy)
    own = q_rows(0)
    z_sum[...] = s_mine[pl.ds(own, block), :] + s_recv[pl.ds(own, block), :]
    for k in range(1, plane):
        remote(x_recv.at[k - 1], x_recv.at[k - 1], x_ss.at[k - 1], x_rs.at[k - 1], pair_dev).wait_recv()
        z_sum[...] += x_recv[k - 1]

    for k in range(1, line):
        first = pl.multiple_of(z_to(k) * piece, piece) if scatter else 0
        copy = remote(
            z_sum.at[pl.ds(first, piece)], z_recv.at[k - 1], z_ss.at[k - 1], z_rs.at[k - 1],
            device(core, q, z_to(k)),
        )
        copy.start()
        sends.append(copy)
    first = pl.multiple_of(z * piece, piece) if scatter else 0
    total = z_sum[pl.ds(first, piece), :]
    for k in range(1, line):
        remote(z_recv.at[k - 1], z_recv.at[k - 1], z_ss.at[k - 1], z_rs.at[k - 1], pair_dev).wait_recv()
        total = total + z_recv[k - 1]

    pieces = line if scatter else 1

    def w_rows(side, q_at, z_at):
        at = side * half + q_at * block + (z_at * piece if scatter else 0)
        return w.at[pl.ds(pl.multiple_of(at, piece), piece)]

    at = core * half + q * block + (z * piece if scatter else 0)
    w[pl.ds(pl.multiple_of(at, piece), piece), :] = (total * (1.0 / math.sqrt(units))).astype(jnp.bfloat16)

    def start(ref, ss, rs, dev):
        copy = remote(ref, ref, ss, rs, dev)
        copy.start()
        sends.append(copy)

    mine = w_rows(core, q, z)
    for k in range(1, pieces):
        start(mine, az_ss.at[k], az_rs.at[k], device(core, q, z_to(k)))
    for kz in range(pieces):
        mine = w_rows(core, q, z_from(kz))
        if kz:
            remote(mine, mine, az_ss.at[kz], az_rs.at[kz], pair_dev).wait_recv()
        for k in range(1, plane):
            start(mine, ax_ss.at[kz, k], ax_rs.at[kz, k], device(core, q_to(k), z))
        start(mine, ac_ss.at[kz, 0], ac_rs.at[kz, 0], pair_dev)
    for kz in range(pieces):
        for k in range(1, plane):
            mine = w_rows(core, q_from(k), z_from(kz))
            remote(mine, mine, ax_ss.at[kz, k], ax_rs.at[kz, k], pair_dev).wait_recv()
            start(mine, ac_ss.at[kz, k], ac_rs.at[kz, k], pair_dev)
    for kz in range(pieces):
        for k in range(plane):
            mine = w_rows(other, q_from(k), z_from(kz))
            remote(mine, mine, ac_ss.at[kz, k], ac_rs.at[kz, k], pair_dev).wait_recv()

    tile = 256 if rows % 256 == 0 else rows
    for first in range(0, rows, tile):
        part = jnp.dot(o_ref[first:first + tile, :], w[...], preferred_element_type=jnp.float32)
        p_ref[first:first + tile, :] = part * (1.0 / math.sqrt(days))
    projected = p_ref[...]
    g_loc[...] = jnp.dot(
        projected.T, projected, precision=HIGHEST, preferred_element_type=jnp.float32
    ) * (1.0 / units)

    gh = rank // 2
    mine_at = pl.multiple_of(core * gh, gh)
    other_at = pl.multiple_of(other * gh, gh)
    copy = remote(g_loc.at[pl.ds(other_at, gh)], g_recv, gc_ss, gc_rs, pair_dev)
    copy.start()
    sends.append(copy)
    copy.wait_recv()
    g_half[...] = g_loc[pl.ds(mine_at, gh), :] + g_recv[...]
    for k in range(1, plane):
        copy = remote(
            g_half, gx_recv.at[q], gx_ss.at[k], gx_rs.at[k], device(core, q_to(k), z)
        )
        copy.start()
        sends.append(copy)
    gx_recv[q] = g_half[...]
    for k in range(1, plane):
        slot = gx_recv.at[q_from(k)]
        remote(slot, slot, gx_ss.at[k], gx_rs.at[k], pair_dev).wait_recv()
    total = gx_recv[0]
    for k in range(1, plane):
        total = total + gx_recv[k]
    g_plane[...] = total
    for k in range(1, line):
        copy = remote(g_plane, gz_recv.at[z], gz_ss.at[k], gz_rs.at[k], device(core, q, z_to(k)))
        copy.start()
        sends.append(copy)
    gz_recv[z] = total
    for k in range(1, line):
        slot = gz_recv.at[z_from(k)]
        remote(slot, slot, gz_ss.at[k], gz_rs.at[k], pair_dev).wait_recv()
    total = gz_recv[0]
    for k in range(1, line):
        total = total + gz_recv[k]
    g_full[pl.ds(mine_at, gh), :] = total
    mine = g_full.at[pl.ds(mine_at, gh)]
    copy = remote(mine, mine, gf_ss, gf_rs, pair_dev)
    copy.start()
    sends.append(copy)
    theirs = g_full.at[pl.ds(other_at, gh)]
    remote(theirs, theirs, gf_ss, gf_rs, pair_dev).wait_recv()
    g_ref[...] = g_full[...]
    for copy in sends:
        copy.wait_send()


def step(sizes, units, outcomes, current):
    rows, days = outcomes.shape
    rank = current.shape[1]
    plane, line, half, block, scatter, piece = plan(sizes, days)
    pieces = line if scatter else 1
    gh = rank // 2
    f32, bf16 = jnp.float32, jnp.bfloat16
    dma = pltpu.SemaphoreType.DMA
    vmem = pl.BlockSpec(memory_space=pltpu.VMEM)
    pair = lambda *n: [dma(n), dma(n)]
    return pl.pallas_call(
        functools.partial(step_kernel, sizes, units),
        out_shape=(
            jax.ShapeDtypeStruct((rows, rank), f32),
            jax.ShapeDtypeStruct((rank, rank), f32),
        ),
        in_specs=[vmem, vmem],
        out_specs=(vmem, vmem),
        scratch_shapes=[
            pltpu.VMEM((rank, rows), bf16),
            pltpu.VMEM((half, rank), f32),
            pltpu.VMEM((half, rank), f32),
            pltpu.VMEM((half, rank), f32),
            pltpu.VMEM((max(plane - 1, 1), block, rank), f32),
            pltpu.VMEM((block, rank), f32),
            pltpu.VMEM((max(line - 1, 1), piece, rank), f32),
            pltpu.VMEM((days, rank), bf16),
            pltpu.VMEM((rank, rank), f32),
            pltpu.VMEM((gh, rank), f32),
            pltpu.VMEM((gh, rank), f32),
            pltpu.VMEM((plane, gh, rank), f32),
            pltpu.VMEM((gh, rank), f32),
            pltpu.VMEM((line, gh, rank), f32),
            pltpu.VMEM((rank, rank), f32),
            *pair(plane), *pair(plane), *pair(line), *pair(line),
            *pair(pieces, plane), *pair(pieces, plane),
            dma, dma, *pair(plane), *pair(line), dma, dma,
        ],
        compiler_params=pltpu.CompilerParams(
            collective_id=0, has_side_effects=True, vmem_limit_bytes=48 * 1024 * 1024
        ),
        name="power_step",
    )(outcomes, current)


def sharp_rsqrt(x):
    r = lax.rsqrt(x)
    return r * (1.5 - 0.5 * ((x * r) * r))


def factor_kernel(p_ref, g_ref, q_ref, r_ref, inv_ref):
    rank = g_ref.shape[0]
    count = rank // PANEL
    row_at = lax.broadcasted_iota(jnp.int32, (PANEL, rank), 0)
    col_at = lax.broadcasted_iota(jnp.int32, (PANEL, rank), 1)
    left = [g_ref[k * PANEL:(k + 1) * PANEL, :] for k in range(count)]
    right = [jnp.where(col_at == row_at + k * PANEL, 1.0, 0.0) for k in range(count)]
    for k in range(count):
        a, b = left[k], right[k]
        cols = [
            jnp.broadcast_to(a[:, k * PANEL + j:k * PANEL + j + 1], (PANEL, rank)) for j in range(PANEL)
        ]
        for j in range(PANEL):
            scale = sharp_rsqrt(jnp.broadcast_to(cols[j][j:j + 1, :], (PANEL, rank)))
            low = jnp.where(row_at > j, cols[j] * scale, 0.0)
            for m in range(j + 1, PANEL):
                cols[m] = cols[m] - low * jnp.broadcast_to(low[m:m + 1, :], (PANEL, rank))
            a_row = jnp.broadcast_to(a[j:j + 1, :], (PANEL, rank)) * scale
            b_row = jnp.broadcast_to(b[j:j + 1, :], (PANEL, rank)) * scale
            here = row_at == j
            a = jnp.where(here, a_row, a - low * a_row)
            b = jnp.where(here, b_row, b - low * b_row)
        r_ref[k * PANEL:(k + 1) * PANEL, :] = jnp.where(col_at >= row_at + k * PANEL, a, 0.0)
        inv_ref[k * PANEL:(k + 1) * PANEL, :] = b
        if k + 1 < count:
            both = jnp.concatenate([a, b], axis=1)
            down = lax.dot_general(
                a, both, (((0,), (0,)), ((), ())), precision=HIGHEST, preferred_element_type=jnp.float32
            )
            for m in range(k + 1, count):
                left[m] = left[m] - down[m * PANEL:(m + 1) * PANEL, :rank]
                right[m] = right[m] - down[m * PANEL:(m + 1) * PANEL, rank:]
    q_ref[...] = lax.dot_general(
        p_ref[...], inv_ref[...], (((1,), (1,)), ((), ())), precision=HIGHEST,
        preferred_element_type=jnp.float32,
    ).astype(q_ref.dtype)


def orthonormalize(projected, gram, dtype):
    rank = gram.shape[0]
    vmem = pl.BlockSpec(memory_space=pltpu.VMEM)
    return pl.pallas_call(
        factor_kernel,
        out_shape=(
            jax.ShapeDtypeStruct(projected.shape, dtype),
            jax.ShapeDtypeStruct((rank, rank), jnp.float32),
        ),
        in_specs=[vmem, vmem],
        out_specs=(vmem, vmem),
        scratch_shapes=[pltpu.VMEM((rank, rank), jnp.float32)],
        name="orthonormalize",
    )(projected, gram)


def per_device(sizes, outcomes, sketch):
    units = outcomes.shape[0] * math.prod(sizes)
    current = sketch
    for power_step in range(POWER):
        last = power_step == POWER - 1
        projected, gram = step(sizes, units, outcomes, current)
        current, factor = orthonormalize(projected, gram, jnp.float32 if last else jnp.bfloat16)
    return current, factor


def solution(mesh):
    return jax.shard_map(
        functools.partial(per_device, tuple(mesh.shape[a] for a in AXES)),
        mesh=mesh,
        in_specs=(P(AXES, None), P(AXES, None)),
        out_specs=(P(AXES, None), P()),
        check_vma=False,
    )
```

```python
import functools
import math

import jax
import jax.numpy as jnp
from jax import lax
from jax.experimental import pallas as pl
from jax.experimental.pallas import tpu as pltpu
from jax.sharding import PartitionSpec as P

POWER = 2
AXES = ("gx", "gy", "gz")
MESH = pl.DeviceIdType.MESH
HIGHEST = lax.Precision.HIGHEST
PANEL = 32


def plan(sizes, days):
    size_x, size_y, size_z = sizes
    plane = (size_x // 2) * size_z
    line = size_y
    half = days // 2
    block = half // plane
    scatter = block % (16 * line) == 0
    piece = block // line if scatter else block
    return plane, line, half, block, scatter, piece


def sharp_rsqrt(x):
    r = lax.rsqrt(x)
    return r * (1.5 - 0.5 * ((x * r) * r))


def factorize(g_ref, r_ref, inv_ref):
    rank = g_ref.shape[0]
    count = rank // PANEL
    row_at = lax.broadcasted_iota(jnp.int32, (PANEL, rank), 0)
    col_at = lax.broadcasted_iota(jnp.int32, (PANEL, rank), 1)
    left = [g_ref[k * PANEL:(k + 1) * PANEL, :] for k in range(count)]
    right = [jnp.where(col_at == row_at + k * PANEL, 1.0, 0.0) for k in range(count)]
    for k in range(count):
        a, b = left[k], right[k]
        cols = [
            jnp.broadcast_to(a[:, k * PANEL + j:k * PANEL + j + 1], (PANEL, rank)) for j in range(PANEL)
        ]
        for j in range(PANEL):
            scale = sharp_rsqrt(jnp.broadcast_to(cols[j][j:j + 1, :], (PANEL, rank)))
            low = jnp.where(row_at > j, cols[j] * scale, 0.0)
            for m in range(j + 1, PANEL):
                cols[m] = cols[m] - low * jnp.broadcast_to(low[m:m + 1, :], (PANEL, rank))
            a_row = jnp.broadcast_to(a[j:j + 1, :], (PANEL, rank)) * scale
            b_row = jnp.broadcast_to(b[j:j + 1, :], (PANEL, rank)) * scale
            here = row_at == j
            a = jnp.where(here, a_row, a - low * a_row)
            b = jnp.where(here, b_row, b - low * b_row)
        if r_ref is not None:
            r_ref[k * PANEL:(k + 1) * PANEL, :] = jnp.where(col_at >= row_at + k * PANEL, a, 0.0)
        inv_ref[k * PANEL:(k + 1) * PANEL, :] = b
        if k + 1 < count:
            both = jnp.concatenate([a, b], axis=1)
            down = lax.dot_general(
                a, both, (((0,), (0,)), ((), ())), precision=HIGHEST, preferred_element_type=jnp.float32
            )
            for m in range(k + 1, count):
                left[m] = left[m] - down[m * PANEL:(m + 1) * PANEL, :rank]
                right[m] = right[m] - down[m * PANEL:(m + 1) * PANEL, rank:]


def times_inverse(x, inv_ref):
    return lax.dot_general(
        x, inv_ref[...], (((1,), (1,)), ((), ())), precision=HIGHEST, preferred_element_type=jnp.float32
    )


def power_kernel(sizes, units, o_hbm, c_ref, q_ref, r_ref, o_ref, o_sem, p_ref, *scratch):
    rows, days = o_ref.shape
    rank = c_ref.shape[1]
    plane, line, half, block, scatter, piece = plan(sizes, days)
    size_z = sizes[2]
    ix, iy, iz = (lax.axis_index(a) for a in AXES)
    core = lax.rem(ix, 2)
    q = lax.div(ix, 2) * size_z + iz
    z = iy

    def device(c_at, q_at, z_at):
        return (lax.div(q_at, size_z) * 2 + c_at, z_at, lax.rem(q_at, size_z))

    other = 1 - core
    pair_dev = device(other, q, z)

    def q_to(k):
        return lax.rem(q + k, plane)

    def q_from(k):
        return lax.rem(q + plane - k, plane)

    def z_to(k):
        return lax.rem(z + k, line)

    def z_from(k):
        return lax.rem(z + line - k, line)

    def remote(src, dst, ss, rs, dev):
        return pltpu.make_async_remote_copy(
            src_ref=src, dst_ref=dst, send_sem=ss, recv_sem=rs, device_id=dev, device_id_type=MESH
        )

    sends = []

    def send(src, dst, ss, rs, dev):
        copy = remote(src, dst, ss, rs, dev)
        copy.start()
        sends.append(copy)

    def arrived(ref, ss, rs):
        remote(ref, ref, ss, rs, pair_dev).wait_recv()

    partners = [pair_dev]
    partners += [device(core, q_to(k), z) for k in range(1, plane)]
    partners += [device(core, q, z_to(k)) for k in range(1, line)]
    barrier = pltpu.get_barrier_semaphore()
    for dev in partners:
        pl.semaphore_signal(barrier, inc=1, device_id=dev, device_id_type=MESH)

    by_block = block % 128 == 0
    order = list(range(1, plane)) + [0]

    def q_rows(k):
        return pl.multiple_of(q_to(k) * block, block)

    def columns(side, first, width):
        return pl.ds(pl.multiple_of(side * half + first, 128), width)

    loads = {}
    if by_block:
        for n, (at_side, k) in enumerate([(1, k) for k in order] + [(0, k) for k in order]):
            cut = columns(other if at_side else core, q_rows(k), block)
            loads[at_side, k] = pltpu.make_async_copy(o_hbm.at[:, cut], o_ref.at[:, cut], o_sem.at[n])
            loads[at_side, k].start()
    else:
        loads[0, 0] = pltpu.make_async_copy(o_hbm, o_ref, o_sem.at[0])
        loads[0, 0].start()
        loads[0, 0].wait()

    per = len(scratch) // POWER
    gram_steps = inverse = p_t = None
    for s in range(POWER):
        (
            ct, s_send, s_recv, s_mine, x_recv, z_sum, z_recv, w,
            g_loc, g_recv, g_half, gx_recv, g_plane, gz_recv, g_full, inv_ref,
            c_ss, c_rs, x_ss, x_rs, z_ss, z_rs, az_ss, az_rs, ax_ss, ax_rs, ac_ss, ac_rs,
            gc_ss, gc_rs, gx_ss, gx_rs, gz_ss, gz_rs, gf_ss, gf_rs,
        ) = scratch[s * per:(s + 1) * per]

        if s == 0:
            ct[:rank, :] = c_ref[...].astype(jnp.float32).T.astype(jnp.bfloat16)
        else:
            high = p_t.astype(jnp.bfloat16)
            ct[:rank, :] = high
            ct[rank:, :] = (p_t - high.astype(jnp.float32)).astype(jnp.bfloat16)

        def product(dst, side, first, width):
            cut = columns(side, first, width)
            now = ct[:rank, :] if s == 0 else ct[...]
            part = jnp.dot(now, o_ref[:, cut], preferred_element_type=jnp.float32)
            if s:
                part = part[:rank] + part[rank:]
            dst[pl.ds(pl.multiple_of(first, 128), width), :] = part.T

        if not by_block:
            for first in range(0, half, 256):
                product(s_send, other, first, min(256, half))
        for n, k in enumerate(order):
            at = q_rows(k)
            if by_block:
                if s == 0:
                    loads[1, k].wait()
                product(s_send, other, at, block)
            if s == 0 and n == 0:
                pl.semaphore_wait(barrier, len(partners))
            send(s_send.at[pl.ds(at, block)], s_recv.at[pl.ds(at, block)], c_ss.at[k], c_rs.at[k], pair_dev)
        if gram_steps:
            gram_steps[0]()
        if not by_block:
            for first in range(0, half, 256):
                product(s_mine, core, first, min(256, half))
        for k in order:
            at = q_rows(k)
            if by_block:
                if s == 0:
                    loads[0, k].wait()
                product(s_mine, core, at, block)
            arrived(s_recv.at[pl.ds(at, block)], c_ss.at[k], c_rs.at[k])
            if k:
                s_mine[pl.ds(at, block), :] += s_recv[pl.ds(at, block), :]
                send(
                    s_mine.at[pl.ds(at, block)], x_recv.at[k - 1], x_ss.at[k - 1], x_rs.at[k - 1],
                    device(core, q_to(k), z),
                )
        if gram_steps:
            gram_steps[1]()
        own = q_rows(0)
        z_sum[...] = s_mine[pl.ds(own, block), :] + s_recv[pl.ds(own, block), :]
        for k in range(1, plane):
            arrived(x_recv.at[k - 1], x_ss.at[k - 1], x_rs.at[k - 1])
            z_sum[...] += x_recv[k - 1]

        for k in range(1, line):
            first = pl.multiple_of(z_to(k) * piece, piece) if scatter else 0
            send(
                z_sum.at[pl.ds(first, piece)], z_recv.at[k - 1], z_ss.at[k - 1], z_rs.at[k - 1],
                device(core, q, z_to(k)),
            )
        if gram_steps:
            gram_steps[2]()
            gram_steps[3]()
            factorize(gram_steps[4], None, inverse)
        first = pl.multiple_of(z * piece, piece) if scatter else 0
        total = z_sum[pl.ds(first, piece), :]
        for k in range(1, line):
            arrived(z_recv.at[k - 1], z_ss.at[k - 1], z_rs.at[k - 1])
            total = total + z_recv[k - 1]
        total = total * (1.0 / math.sqrt(units))
        if inverse is not None:
            total = times_inverse(total, inverse)

        pieces = line if scatter else 1

        def w_rows(side, q_at, z_at):
            at = side * half + q_at * block + (z_at * piece if scatter else 0)
            return w.at[pl.ds(pl.multiple_of(at, piece), piece)]

        at = core * half + q * block + (z * piece if scatter else 0)
        w[pl.ds(pl.multiple_of(at, piece), piece), :] = total.astype(jnp.bfloat16)

        mine = w_rows(core, q, z)
        for k in range(1, pieces):
            send(mine, mine, az_ss.at[k], az_rs.at[k], device(core, q, z_to(k)))
        for kz in range(pieces):
            mine = w_rows(core, q, z_from(kz))
            if kz:
                arrived(mine, az_ss.at[kz], az_rs.at[kz])
            for k in range(1, plane):
                send(mine, mine, ax_ss.at[kz, k], ax_rs.at[kz, k], device(core, q_to(k), z))
            send(mine, mine, ac_ss.at[kz, 0], ac_rs.at[kz, 0], pair_dev)
        for kz in range(pieces):
            for k in range(1, plane):
                mine = w_rows(core, q_from(k), z_from(kz))
                arrived(mine, ax_ss.at[kz, k], ax_rs.at[kz, k])
                send(mine, mine, ac_ss.at[kz, k], ac_rs.at[kz, k], pair_dev)
        for kz in range(pieces):
            for k in range(plane):
                arrived(w_rows(other, q_from(k), z_from(kz)), ac_ss.at[kz, k], ac_rs.at[kz, k])

        tile = 256 if rows % 256 == 0 else rows
        for first in range(0, rows, tile):
            part = jnp.dot(o_ref[first:first + tile, :], w[...], preferred_element_type=jnp.float32)
            p_ref[first:first + tile, :] = part * (1.0 / math.sqrt(days))
        projected = p_ref[...]
        p_t = projected.T
        g_loc[...] = jnp.dot(
            p_t, projected, precision=HIGHEST, preferred_element_type=jnp.float32
        ) * (1.0 / units)

        gh = rank // 2
        mine_at = pl.multiple_of(core * gh, gh)
        other_at = pl.multiple_of(other * gh, gh)
        send(g_loc.at[pl.ds(other_at, gh)], g_recv, gc_ss.at[0], gc_rs.at[0], pair_dev)

        def gram_plane_out(g_recv=g_recv, gc_ss=gc_ss, gc_rs=gc_rs, g_half=g_half, g_loc=g_loc,
                           gx_recv=gx_recv, gx_ss=gx_ss, gx_rs=gx_rs):
            arrived(g_recv, gc_ss.at[0], gc_rs.at[0])
            g_half[...] = g_loc[pl.ds(mine_at, gh), :] + g_recv[...]
            for k in range(1, plane):
                send(g_half, gx_recv.at[q], gx_ss.at[k], gx_rs.at[k], device(core, q_to(k), z))

        def gram_line_out(g_half=g_half, gx_recv=gx_recv, gx_ss=gx_ss, gx_rs=gx_rs, g_plane=g_plane,
                          gz_recv=gz_recv, gz_ss=gz_ss, gz_rs=gz_rs):
            gx_recv[q] = g_half[...]
            for k in range(1, plane):
                arrived(gx_recv.at[q_from(k)], gx_ss.at[k], gx_rs.at[k])
            total = gx_recv[0]
            for k in range(1, plane):
                total = total + gx_recv[k]
            g_plane[...] = total
            for k in range(1, line):
                send(g_plane, gz_recv.at[z], gz_ss.at[k], gz_rs.at[k], device(core, q, z_to(k)))

        def gram_pair_out(g_plane=g_plane, gz_recv=gz_recv, gz_ss=gz_ss, gz_rs=gz_rs, g_full=g_full,
                          gf_ss=gf_ss, gf_rs=gf_rs):
            gz_recv[z] = g_plane[...]
            for k in range(1, line):
                arrived(gz_recv.at[z_from(k)], gz_ss.at[k], gz_rs.at[k])
            total = gz_recv[0]
            for k in range(1, line):
                total = total + gz_recv[k]
            g_full[pl.ds(mine_at, gh), :] = total
            mine = g_full.at[pl.ds(mine_at, gh)]
            send(mine, mine, gf_ss.at[0], gf_rs.at[0], pair_dev)

        def gram_done(g_full=g_full, gf_ss=gf_ss, gf_rs=gf_rs):
            arrived(g_full.at[pl.ds(other_at, gh)], gf_ss.at[0], gf_rs.at[0])

        gram_steps = (gram_plane_out, gram_line_out, gram_pair_out, gram_done, g_full)
        inverse = inv_ref

    for part in gram_steps[:4]:
        part()
    factorize(gram_steps[4], r_ref, inverse)
    q_ref[...] = times_inverse(p_ref[...], inverse)
    for copy in sends:
        copy.wait_send()


def per_device(sizes, outcomes, sketch):
    rows, days = outcomes.shape
    rank = sketch.shape[1]
    units = rows * math.prod(sizes)
    plane, line, half, block, scatter, piece = plan(sizes, days)
    pieces = line if scatter else 1
    gh = rank // 2
    f32, bf16 = jnp.float32, jnp.bfloat16
    dma = pltpu.SemaphoreType.DMA
    vmem = pl.BlockSpec(memory_space=pltpu.VMEM)
    pair = lambda *n: [dma(n), dma(n)]
    one_step = [
        pltpu.VMEM((2 * rank, rows), bf16),
        pltpu.VMEM((half, rank), f32),
        pltpu.VMEM((half, rank), f32),
        pltpu.VMEM((half, rank), f32),
        pltpu.VMEM((max(plane - 1, 1), block, rank), f32),
        pltpu.VMEM((block, rank), f32),
        pltpu.VMEM((max(line - 1, 1), piece, rank), f32),
        pltpu.VMEM((days, rank), bf16),
        pltpu.VMEM((rank, rank), f32),
        pltpu.VMEM((gh, rank), f32),
        pltpu.VMEM((gh, rank), f32),
        pltpu.VMEM((plane, gh, rank), f32),
        pltpu.VMEM((gh, rank), f32),
        pltpu.VMEM((line, gh, rank), f32),
        pltpu.VMEM((rank, rank), f32),
        pltpu.VMEM((rank, rank), f32),
        *pair(plane), *pair(plane), *pair(line), *pair(line),
        *pair(pieces, plane), *pair(pieces, plane),
        *pair(1), *pair(plane), *pair(line), *pair(1),
    ]
    return pl.pallas_call(
        functools.partial(power_kernel, sizes, units),
        out_shape=(
            jax.ShapeDtypeStruct((rows, rank), f32),
            jax.ShapeDtypeStruct((rank, rank), f32),
        ),
        in_specs=[pl.BlockSpec(memory_space=pltpu.HBM), vmem],
        out_specs=(vmem, vmem),
        scratch_shapes=[
            pltpu.VMEM((rows, days), bf16),
            dma((2 * plane,)),
            pltpu.VMEM((rows, rank), f32),
            *(one_step * POWER),
        ],
        compiler_params=pltpu.CompilerParams(
            collective_id=0, has_side_effects=True, vmem_limit_bytes=48 * 1024 * 1024
        ),
        name="power_steps",
    )(outcomes, sketch)


def solution(mesh):
    return jax.shard_map(
        functools.partial(per_device, tuple(mesh.shape[a] for a in AXES)),
        mesh=mesh,
        in_specs=(P(AXES, None), P(AXES, None)),
        out_specs=(P(AXES, None), P()),
        check_vma=False,
    )
```

```python
import functools
import math

import jax
import jax.numpy as jnp
from jax import lax
from jax.experimental import pallas as pl
from jax.experimental.pallas import tpu as pltpu
from jax.sharding import PartitionSpec as P

POWER = 2
AXES = ("gx", "gy", "gz")
MESH = pl.DeviceIdType.MESH
HIGHEST = lax.Precision.HIGHEST
PANEL = 32


def plan(sizes, days):
    size_x, size_y, size_z = sizes
    plane = (size_x // 2) * size_z
    line = size_y
    half = days // 2
    block = half // plane
    scatter = block % (16 * line) == 0
    piece = block // line if scatter else block
    return plane, line, half, block, scatter, piece


def factorize(g_ref, r_ref, inv_ref):
    rank = g_ref.shape[0]
    count = rank // PANEL
    row_at = lax.broadcasted_iota(jnp.int32, (PANEL, rank), 0)
    col_at = lax.broadcasted_iota(jnp.int32, (PANEL, rank), 1)
    left = [g_ref[k * PANEL:(k + 1) * PANEL, :] for k in range(count)]
    right = [jnp.where(col_at == row_at + k * PANEL, 1.0, 0.0) for k in range(count)]
    for k in range(count):
        a, b = left[k], right[k]
        cols = [
            jnp.broadcast_to(a[:, k * PANEL + j:k * PANEL + j + 1], (PANEL, rank)) for j in range(PANEL)
        ]
        scales = jnp.zeros((PANEL, rank), jnp.float32)
        for j in range(PANEL):
            pivot = jnp.broadcast_to(cols[j][j:j + 1, :], (PANEL, rank))
            root = lax.rsqrt(pivot)
            inv = root * root
            inv = inv * (2.0 - pivot * inv)
            below = jnp.where(row_at > j, cols[j], 0.0)
            low = below * inv
            for m in range(j + 1, PANEL):
                cols[m] = cols[m] - low * jnp.broadcast_to(cols[j][m:m + 1, :], (PANEL, rank))
            scales = jnp.where(row_at == j, root * (1.5 - 0.5 * ((pivot * root) * root)), scales)
            a = a - low * jnp.broadcast_to(a[j:j + 1, :], (PANEL, rank))
            b = b - low * jnp.broadcast_to(b[j:j + 1, :], (PANEL, rank))
        a, b = a * scales, b * scales
        if r_ref is not None:
            r_ref[k * PANEL:(k + 1) * PANEL, :] = jnp.where(col_at >= row_at + k * PANEL, a, 0.0)
        inv_ref[k * PANEL:(k + 1) * PANEL, :] = b
        if k + 1 < count:
            both = jnp.concatenate([a, b], axis=1)
            down = lax.dot_general(
                a, both, (((0,), (0,)), ((), ())), precision=HIGHEST, preferred_element_type=jnp.float32
            )
            for m in range(k + 1, count):
                left[m] = left[m] - down[m * PANEL:(m + 1) * PANEL, :rank]
                right[m] = right[m] - down[m * PANEL:(m + 1) * PANEL, rank:]


def times_inverse(x, inv_ref):
    return lax.dot_general(
        x, inv_ref[...], (((1,), (1,)), ((), ())), precision=HIGHEST, preferred_element_type=jnp.float32
    )


def power_kernel(sizes, units, o_hbm, c_ref, q_ref, r_ref, o_ref, o_sem, p_ref, *scratch):
    rows, days = o_ref.shape
    rank = c_ref.shape[1]
    plane, line, half, block, scatter, piece = plan(sizes, days)
    size_z = sizes[2]
    ix, iy, iz = (lax.axis_index(a) for a in AXES)
    core = lax.rem(ix, 2)
    q = lax.div(ix, 2) * size_z + iz
    z = iy

    def device(c_at, q_at, z_at):
        return (lax.div(q_at, size_z) * 2 + c_at, z_at, lax.rem(q_at, size_z))

    other = 1 - core
    pair_dev = device(other, q, z)

    def q_to(k):
        return lax.rem(q + k, plane)

    def q_from(k):
        return lax.rem(q + plane - k, plane)

    def z_to(k):
        return lax.rem(z + k, line)

    def z_from(k):
        return lax.rem(z + line - k, line)

    def remote(src, dst, ss, rs, dev):
        return pltpu.make_async_remote_copy(
            src_ref=src, dst_ref=dst, send_sem=ss, recv_sem=rs, device_id=dev, device_id_type=MESH
        )

    sends = []

    def send(src, dst, ss, rs, dev):
        copy = remote(src, dst, ss, rs, dev)
        copy.start()
        sends.append(copy)

    def arrived(ref, ss, rs):
        remote(ref, ref, ss, rs, pair_dev).wait_recv()

    partners = [pair_dev]
    partners += [device(core, q_to(k), z) for k in range(1, plane)]
    partners += [device(core, q, z_to(k)) for k in range(1, line)]
    barrier = pltpu.get_barrier_semaphore()
    for dev in partners:
        pl.semaphore_signal(barrier, inc=1, device_id=dev, device_id_type=MESH)

    by_block = block % 128 == 0
    order = list(range(1, plane)) + [0]

    def q_rows(k):
        return pl.multiple_of(q_to(k) * block, block)

    def columns(side, first, width):
        return pl.ds(pl.multiple_of(side * half + first, 128), width)

    turns = [(1, order[0])]
    for n in range(1, plane):
        turns += [(1, order[n]), (0, order[n - 1])]
    turns += [(0, order[-1])]
    loads = {}
    if by_block:
        for n, (at_side, k) in enumerate(turns):
            cut = columns(other if at_side else core, q_rows(k), block)
            loads[at_side, k] = pltpu.make_async_copy(o_hbm.at[:, cut], o_ref.at[:, cut], o_sem.at[n])
            loads[at_side, k].start()
    else:
        loads[0, 0] = pltpu.make_async_copy(o_hbm, o_ref, o_sem.at[0])
        loads[0, 0].start()
        loads[0, 0].wait()

    per = len(scratch) // POWER
    gram_steps = inverse = p_t = None
    for s in range(POWER):
        (
            ct, s_send, s_recv, s_mine, x_recv, z_sum, z_recv, w,
            g_loc, g_recv, g_half, gx_recv, g_plane, gz_recv, g_full, inv_ref,
            c_ss, c_rs, x_ss, x_rs, z_ss, z_rs, az_ss, az_rs, ax_ss, ax_rs, ac_ss, ac_rs,
            gc_ss, gc_rs, gx_ss, gx_rs, gz_ss, gz_rs, gf_ss, gf_rs,
        ) = scratch[s * per:(s + 1) * per]

        if s == 0:
            ct[:rank, :] = c_ref[...].astype(jnp.float32).T.astype(jnp.bfloat16)
        else:
            high = p_t.astype(jnp.bfloat16)
            ct[:rank, :] = high
            ct[rank:, :] = (p_t - high.astype(jnp.float32)).astype(jnp.bfloat16)

        def product(dst, side, first, width):
            cut = columns(side, first, width)
            now = ct[:rank, :] if s == 0 else ct[...]
            part = jnp.dot(now, o_ref[:, cut], preferred_element_type=jnp.float32)
            if s:
                part = part[:rank] + part[rank:]
            dst[pl.ds(pl.multiple_of(first, 128), width), :] = part.T

        if not by_block:
            for first in range(0, half, 256):
                product(s_send, other, first, min(256, half))
                product(s_mine, core, first, min(256, half))
        for n, (at_side, k) in enumerate(turns):
            at = q_rows(k)
            if by_block:
                if s == 0:
                    loads[at_side, k].wait()
                product(s_send if at_side else s_mine, other if at_side else core, at, block)
            if s == 0 and n == 0:
                pl.semaphore_wait(barrier, len(partners))
            if at_side:
                send(
                    s_send.at[pl.ds(at, block)], s_recv.at[pl.ds(at, block)], c_ss.at[k], c_rs.at[k], pair_dev
                )
            else:
                arrived(s_recv.at[pl.ds(at, block)], c_ss.at[k], c_rs.at[k])
                if k:
                    s_mine[pl.ds(at, block), :] += s_recv[pl.ds(at, block), :]
                    send(
                        s_mine.at[pl.ds(at, block)], x_recv.at[k - 1], x_ss.at[k - 1], x_rs.at[k - 1],
                        device(core, q_to(k), z),
                    )
            if gram_steps and n == min(2, len(turns) - 1):
                gram_steps[0]()
        if gram_steps:
            gram_steps[1]()
        own = q_rows(0)
        z_sum[...] = s_mine[pl.ds(own, block), :] + s_recv[pl.ds(own, block), :]
        for k in range(1, plane):
            arrived(x_recv.at[k - 1], x_ss.at[k - 1], x_rs.at[k - 1])
            z_sum[...] += x_recv[k - 1]

        for k in range(1, line):
            first = pl.multiple_of(z_to(k) * piece, piece) if scatter else 0
            send(
                z_sum.at[pl.ds(first, piece)], z_recv.at[k - 1], z_ss.at[k - 1], z_rs.at[k - 1],
                device(core, q, z_to(k)),
            )
        if gram_steps:
            gram_steps[2]()
            gram_steps[3]()
            factorize(gram_steps[4], None, inverse)
        first = pl.multiple_of(z * piece, piece) if scatter else 0
        total = z_sum[pl.ds(first, piece), :]
        for k in range(1, line):
            arrived(z_recv.at[k - 1], z_ss.at[k - 1], z_rs.at[k - 1])
            total = total + z_recv[k - 1]
        total = total * (1.0 / math.sqrt(units))
        if inverse is not None:
            total = times_inverse(total, inverse)

        pieces = line if scatter else 1

        def w_rows(side, q_at, z_at):
            at = side * half + q_at * block + (z_at * piece if scatter else 0)
            return w.at[pl.ds(pl.multiple_of(at, piece), piece)]

        at = core * half + q * block + (z * piece if scatter else 0)
        w[pl.ds(pl.multiple_of(at, piece), piece), :] = total.astype(jnp.bfloat16)

        mine = w_rows(core, q, z)
        for k in range(1, pieces):
            send(mine, mine, az_ss.at[k], az_rs.at[k], device(core, q, z_to(k)))
        for kz in range(pieces):
            mine = w_rows(core, q, z_from(kz))
            if kz:
                arrived(mine, az_ss.at[kz], az_rs.at[kz])
            for k in range(1, plane):
                send(mine, mine, ax_ss.at[kz, k], ax_rs.at[kz, k], device(core, q_to(k), z))
            send(mine, mine, ac_ss.at[kz, 0], ac_rs.at[kz, 0], pair_dev)
        for kz in range(pieces):
            for k in range(1, plane):
                mine = w_rows(core, q_from(k), z_from(kz))
                arrived(mine, ax_ss.at[kz, k], ax_rs.at[kz, k])
                send(mine, mine, ac_ss.at[kz, k], ac_rs.at[kz, k], pair_dev)
        for kz in range(pieces):
            for k in range(plane):
                arrived(w_rows(other, q_from(k), z_from(kz)), ac_ss.at[kz, k], ac_rs.at[kz, k])

        tile = 256 if rows % 256 == 0 else rows
        for first in range(0, rows, tile):
            part = jnp.dot(o_ref[first:first + tile, :], w[...], preferred_element_type=jnp.float32)
            p_ref[first:first + tile, :] = part * (1.0 / math.sqrt(days))
        projected = p_ref[...]
        p_t = projected.T
        g_loc[...] = jnp.dot(
            p_t, projected, precision=HIGHEST, preferred_element_type=jnp.float32
        ) * (1.0 / units)

        gh = rank // 2
        mine_at = pl.multiple_of(core * gh, gh)
        other_at = pl.multiple_of(other * gh, gh)
        send(g_loc.at[pl.ds(other_at, gh)], g_recv, gc_ss.at[0], gc_rs.at[0], pair_dev)

        def gram_plane_out(g_recv=g_recv, gc_ss=gc_ss, gc_rs=gc_rs, g_half=g_half, g_loc=g_loc,
                           gx_recv=gx_recv, gx_ss=gx_ss, gx_rs=gx_rs):
            arrived(g_recv, gc_ss.at[0], gc_rs.at[0])
            g_half[...] = g_loc[pl.ds(mine_at, gh), :] + g_recv[...]
            for k in range(1, plane):
                send(g_half, gx_recv.at[q], gx_ss.at[k], gx_rs.at[k], device(core, q_to(k), z))

        def gram_line_out(g_half=g_half, gx_recv=gx_recv, gx_ss=gx_ss, gx_rs=gx_rs, g_plane=g_plane,
                          gz_recv=gz_recv, gz_ss=gz_ss, gz_rs=gz_rs):
            gx_recv[q] = g_half[...]
            for k in range(1, plane):
                arrived(gx_recv.at[q_from(k)], gx_ss.at[k], gx_rs.at[k])
            total = gx_recv[0]
            for k in range(1, plane):
                total = total + gx_recv[k]
            g_plane[...] = total
            for k in range(1, line):
                send(g_plane, gz_recv.at[z], gz_ss.at[k], gz_rs.at[k], device(core, q, z_to(k)))

        def gram_pair_out(g_plane=g_plane, gz_recv=gz_recv, gz_ss=gz_ss, gz_rs=gz_rs, g_full=g_full,
                          gf_ss=gf_ss, gf_rs=gf_rs):
            gz_recv[z] = g_plane[...]
            for k in range(1, line):
                arrived(gz_recv.at[z_from(k)], gz_ss.at[k], gz_rs.at[k])
            total = gz_recv[0]
            for k in range(1, line):
                total = total + gz_recv[k]
            g_full[pl.ds(mine_at, gh), :] = total
            mine = g_full.at[pl.ds(mine_at, gh)]
            send(mine, mine, gf_ss.at[0], gf_rs.at[0], pair_dev)

        def gram_done(g_full=g_full, gf_ss=gf_ss, gf_rs=gf_rs):
            arrived(g_full.at[pl.ds(other_at, gh)], gf_ss.at[0], gf_rs.at[0])

        gram_steps = (gram_plane_out, gram_line_out, gram_pair_out, gram_done, g_full)
        inverse = inv_ref

    for part in gram_steps[:4]:
        part()
    factorize(gram_steps[4], r_ref, inverse)
    q_ref[...] = times_inverse(p_ref[...], inverse)
    for copy in sends:
        copy.wait_send()


def per_device(sizes, outcomes, sketch):
    rows, days = outcomes.shape
    rank = sketch.shape[1]
    units = rows * math.prod(sizes)
    plane, line, half, block, scatter, piece = plan(sizes, days)
    pieces = line if scatter else 1
    gh = rank // 2
    f32, bf16 = jnp.float32, jnp.bfloat16
    dma = pltpu.SemaphoreType.DMA
    vmem = pl.BlockSpec(memory_space=pltpu.VMEM)
    pair = lambda *n: [dma(n), dma(n)]
    one_step = [
        pltpu.VMEM((2 * rank, rows), bf16),
        pltpu.VMEM((half, rank), f32),
        pltpu.VMEM((half, rank), f32),
        pltpu.VMEM((half, rank), f32),
        pltpu.VMEM((max(plane - 1, 1), block, rank), f32),
        pltpu.VMEM((block, rank), f32),
        pltpu.VMEM((max(line - 1, 1), piece, rank), f32),
        pltpu.VMEM((days, rank), bf16),
        pltpu.VMEM((rank, rank), f32),
        pltpu.VMEM((gh, rank), f32),
        pltpu.VMEM((gh, rank), f32),
        pltpu.VMEM((plane, gh, rank), f32),
        pltpu.VMEM((gh, rank), f32),
        pltpu.VMEM((line, gh, rank), f32),
        pltpu.VMEM((rank, rank), f32),
        pltpu.VMEM((rank, rank), f32),
        *pair(plane), *pair(plane), *pair(line), *pair(line),
        *pair(pieces, plane), *pair(pieces, plane),
        *pair(1), *pair(plane), *pair(line), *pair(1),
    ]
    return pl.pallas_call(
        functools.partial(power_kernel, sizes, units),
        out_shape=(
            jax.ShapeDtypeStruct((rows, rank), f32),
            jax.ShapeDtypeStruct((rank, rank), f32),
        ),
        in_specs=[pl.BlockSpec(memory_space=pltpu.HBM), vmem],
        out_specs=(vmem, vmem),
        scratch_shapes=[
            pltpu.VMEM((rows, days), bf16),
            dma((2 * plane,)),
            pltpu.VMEM((rows, rank), f32),
            *(one_step * POWER),
        ],
        compiler_params=pltpu.CompilerParams(
            collective_id=0, has_side_effects=True, vmem_limit_bytes=63 * 1024 * 1024
        ),
        name="power_steps",
    )(outcomes, sketch)


def solution(mesh):
    return jax.shard_map(
        functools.partial(per_device, tuple(mesh.shape[a] for a in AXES)),
        mesh=mesh,
        in_specs=(P(AXES, None), P(AXES, None)),
        out_specs=(P(AXES, None), P()),
        check_vma=False,
    )
```
